32 devices in a mesh: dp: 4 (over y, x), vocab: 8 (over z, core).
Axes of the slice: x: 2, y: 2, z: 4, core: 2. Of those that a mesh axis runs over, the one named last changes fastest.
Arguments:
- hidden: bfloat16 [256, 3072], P(('dp', 'vocab')), parts along dimension 0, may hold values from -60 to 60
- weight: bfloat16 [3072, 8192], P(None, 'vocab'), may hold values from -0.32421875 to 0.32421875
- targets: int32 [256], P('dp'), parts along dimension 0, may hold values from 0 to 8191
Outputs:
- loss: float32 [4], P('dp'), parts along dimension 0
- d_hidden: bfloat16 [256, 3072], P(('dp', 'vocab')), parts along dimension 0
- d_weight: bfloat16 [12288, 8192], P('dp', 'vocab'), parts along dimension 0
The draws below stay inside these ranges and needn't reach their ends.
There are 4 independent parts, one for each index of `dp`. The reference program is written for one: setup_inputs(seed, part) draws one part's arguments, and reference() takes and returns one part's arrays. A program takes and returns all parts, laid end to end along the dimension named above; an argument that names none is the same for every part. Nothing has to cross between parts.
All inputs are finite; a program needn't handle non-finite values.
Results may differ from the reference program's by a relative error of at most 0.0035.
Values may be sent and summed in bfloat16 or wider, within the bound.
A program may use at most 64 MiB of HBM per device.

```python
import jax
import jax.numpy as jnp
from jax import lax

D = 3072
TOKENS = 64
VOCAB = 8192


def draw_hidden(key, part):
    first = jax.random.fold_in(jax.random.fold_in(key, 17), 0)
    values = jax.random.normal(first, (TOKENS, D), jnp.float32)
    return jnp.clip(values, -60.0, 60.0).astype(jnp.bfloat16)


def touch_ends(result, own_key, low, top_value):
    place = [jax.random.randint(jax.random.fold_in(own_key, axis), (), 0, length) for axis, length in enumerate(result.shape)]
    main_axis = result.shape.index(max(result.shape))
    neighbour = place[:main_axis] + [(place[main_axis] + 1) % result.shape[main_axis]] + place[main_axis + 1:]
    return result.at[tuple(place)].set(low).at[tuple(neighbour)].set(top_value)


def levels(key, dims, shards, least, high):
    level = 1.0
    for axis_at, parts in shards:
        steps = jax.random.uniform(jax.random.fold_in(jax.random.fold_in(key, 6), axis_at), (parts,), jnp.float32, least / len(shards), high / len(shards))
        level = level * jnp.repeat(jnp.exp(steps), dims[axis_at] // parts).reshape((-1,) + (1,) * (len(dims) - 1 - axis_at))
    return level


def noise(rng, extent, width, most, shards=(), kind=jnp.bfloat16):
    drawn = width * jax.random.normal(rng, extent, jnp.float32)
    if shards:
        drawn = drawn * levels(rng, extent, shards, -0.22, 0.18)
    return jnp.clip(drawn, -most, most).astype(kind)


def setup_inputs(seed: int = 0, part: int = 0) -> dict:
    key_list = jax.random.split(jax.random.key(seed), 4)
    part_keys = jax.random.split(jax.random.fold_in(key_list[3], part), 4)
    hidden = draw_hidden(jax.random.fold_in(jax.random.fold_in(key_list[3], part), 71), part)
    weight = noise(key_list[1], (D, VOCAB), (3 / D ** 0.5), 0.32421875, ((1, 8),))
    targets = touch_ends(jax.random.randint(part_keys[2], (TOKENS,), 0, VOCAB), jax.random.fold_in(part_keys[2], 1), 0, VOCAB - 1).astype(jnp.int32)
    return dict(hidden=hidden, weight=weight, targets=targets)


def reference(hidden, weight, targets):
    logits = jnp.dot(hidden, weight, preferred_element_type=jnp.float32)
    top = jnp.max(logits, axis=1)
    expo = jnp.exp(logits - top[:, None])
    total = jnp.sum(expo, axis=1)
    columns = lax.broadcasted_iota(jnp.int32, logits.shape, 1)
    hits = columns == targets.astype(jnp.int32)[:, None]
    picked = jnp.sum(jnp.where(hits, logits, jnp.zeros_like(logits)), axis=1)
    loss = jnp.mean(top + jnp.log(total) - picked).reshape(1)
    grad_logits = (expo / total[:, None] - hits.astype(logits.dtype)).astype(jnp.bfloat16)
    d_hidden = lax.dot_general(grad_logits, weight, (((1,), (1,)), ((), ())), preferred_element_type=jnp.float32).astype(jnp.bfloat16)
    d_weight = lax.dot_general(hidden, grad_logits, (((0,), (0,)), ((), ())), preferred_element_type=jnp.float32).astype(jnp.bfloat16)
    return loss, d_hidden, d_weight
```

```python
import functools

import jax
import jax.numpy as jnp
from jax import lax
from jax.experimental import pallas as pl
from jax.experimental.pallas import tpu as pltpu
from jax.sharding import PartitionSpec as P

MESH = pl.DeviceIdType.MESH
F32 = jnp.float32
BF16 = jnp.bfloat16
ACROSS = (((1,), (1,)), ((), ()))
DOWN = (((0,), (0,)), ((), ()))


def split(length, most, unit):
    for parts in range(most, 0, -1):
        if length % (parts * unit) == 0:
            return parts
    return 1


def remote(src, dst, send, recv, device):
    return pltpu.make_async_remote_copy(
        src_ref=src, dst_ref=dst, send_sem=send, recv_sem=recv, device_id={"vocab": device}, device_id_type=MESH
    )


def loss_kernel(
    n, h_hbm, w_hbm, t_hbm, dw_ref, dh_ref, loss_ref,
    t_ref, aim_ref, hid_ref, g_ref, w_v, slots, e_v, stats, near, scale, mix, part, xbuf, outb, rbuf,
    goal, goal_in, goal_sum, goal_far,
    in_sem, w_sem, send_sem, ag_recv, fw_recv, recv_sem, x_recv,
):
    me = lax.axis_index("vocab")
    chips = n // 2
    chip, core = me // 2, me % 2
    partner = chip * 2 + (1 - core)
    pieces, rows, span = slots.shape[0], slots.shape[3], slots.shape[4]
    tokens, width = e_v.shape
    depth = w_v.shape[0]
    parts, wide = part.shape[0], part.shape[4]
    blocks = split(depth, 6, 256)
    tall = depth // blocks
    ag_send, fw_send, st_send, near_send, x_send, rs_send, goal_send, far_send = [send_sem.at[i] for i in range(8)]
    st_recv, near_recv, rs_recv, goal_recv, far_recv = [recv_sem.at[i] for i in range(5)]

    above = chips - 1 - chip

    def other(k):
        up = (above - k + chips) // chips
        return up * (chips - k) + (1 - up) * (k - 1 - above)

    takes = [
        pltpu.make_async_copy(h_hbm.at[:, pl.ds(a * span, span)], slots.at[a, core, chip], in_sem.at[a])
        for a in range(pieces)
    ]
    takes.append(pltpu.make_async_copy(t_hbm, t_ref, in_sem.at[pieces]))
    for take in takes:
        take.start()
    loads = [
        pltpu.make_async_copy(w_hbm.at[pl.ds(a * span, span), :], w_v.at[pl.ds(a * span, span), :], w_sem.at[a])
        for a in range(pieces)
    ]
    for load in loads:
        load.start()

    barrier = pltpu.get_barrier_semaphore()
    for k in range(1, n):
        pl.semaphore_signal(barrier, inc=1, device_id={"vocab": lax.rem(me + k, n)}, device_id_type=MESH)
    for take in takes:
        take.wait()
    aim_ref[...] = jnp.transpose(jnp.broadcast_to((t_ref[...] - me * width).astype(F32), (128, tokens)))
    pl.semaphore_wait(barrier, n - 1)

    for a in range(pieces):
        own = slots.at[a, core, chip]
        for k in range(1, chips):
            remote(own, own, ag_send, ag_recv.at[a], other(k) * 2 + core).start()

    hits = lax.broadcasted_iota(jnp.int32, (tokens, width), 1).astype(F32) == aim_ref[:, 0:1]
    g_ref[...] = hits.astype(F32).astype(BF16)
    for load in loads:
        load.wait()
    for j in range(parts):
        term = lax.dot_general(g_ref[...], w_v[j * wide:(j + 1) * wide, :], ACROSS, preferred_element_type=F32)
        for z in range(chips):
            for half in range(2):
                at = (2 * z + half) * rows
                goal[half, z, :, j * wide:(j + 1) * wide] = term[at:at + rows, :].astype(BF16)
    goal_copy = remote(goal.at[1 - core], goal_in, goal_send, goal_recv, partner)
    goal_copy.start()
    goal_copy.wait_recv()
    for z in range(chips):
        goal_sum[z] = (goal[core, z].astype(F32) + goal_in[z].astype(F32)).astype(BF16)
    for k in range(1, chips):
        remote(goal_sum.at[other(k)], goal_far.at[chip], far_send, far_recv, other(k) * 2 + core).start()

    def finish(a):
        remote(slots.at[a, 1 - core], slots.at[a, 1 - core], fw_send, fw_recv.at[a], partner).wait_recv()
        for z in range(chips):
            both = jnp.concatenate([slots[a, 0, z].astype(F32), slots[a, 1, z].astype(F32)], axis=0)
            hid_ref[2 * rows * z:2 * rows * (z + 1), a * span:(a + 1) * span] = both.astype(BF16)
        term = jnp.dot(
            hid_ref[:, a * span:(a + 1) * span], w_v[a * span:(a + 1) * span, :], preferred_element_type=F32
        )
        if a == 0:
            e_v[...] = term
        else:
            e_v[...] += term

    for a in range(pieces):
        there = slots.at[a, core, pl.ds(0, chips - 1)]
        remote(there, there, ag_send, ag_recv.at[a], partner).wait_recv()
        remote(slots.at[a, core], slots.at[a, core], fw_send, fw_recv.at[a], partner).start()
        if a > 0:
            finish(a - 1)
    finish(pieces - 1)

    logits = e_v[...]
    hits = lax.broadcasted_iota(jnp.int32, (tokens, width), 1).astype(F32) == aim_ref[:, 0:1]
    local_top = jnp.max(logits, axis=1, keepdims=True)
    expo = jnp.exp(logits - local_top)
    e_v[...] = expo
    g_ref[...] = jnp.where(hits, 0.0, expo).astype(BF16)
    local_total = jnp.sum(expo, axis=1, keepdims=True)
    local_picked = jnp.sum(jnp.where(hits, logits, 0.0), axis=1, keepdims=True)
    lane = lax.broadcasted_iota(jnp.int32, (tokens, 128), 1)
    packed = jnp.where(lane == 0, local_top, jnp.where(lane == 1, local_total, local_picked))
    near[0] = packed
    near_copy = remote(near.at[0], near.at[1], near_send, near_recv, partner)
    near_copy.start()
    stats[me] = jnp.transpose(packed)[0:8, :]
    for k in range(1, n):
        remote(stats.at[me], stats.at[me], st_send, st_recv, lax.rem(me + k, n)).start()

    def pair_copy(j):
        return remote(part.at[j, 1 - core], xbuf.at[j], x_send, x_recv.at[j], partner)

    def chip_sum(j, z):
        return (
            part[j, core, z] * scale[0, core, z][:, 0:1] + xbuf[j, z] * scale[1, core, z][:, 0:1]
        )

    def pass_on(j):
        pair_copy(j).wait_recv()
        for z in range(chips):
            outb[j, z] = chip_sum(j, z).astype(BF16)
        for k in range(1, chips):
            remote(outb.at[j, other(k)], rbuf.at[j, chip], rs_send, rs_recv, other(k) * 2 + core).start()

    for j in range(parts):
        term = lax.dot_general(g_ref[...], w_v[j * wide:(j + 1) * wide, :], ACROSS, preferred_element_type=F32)
        for z in range(chips):
            for half in range(2):
                at = (2 * z + half) * rows
                part[j, half, z] = term[at:at + rows, :]
        pair_copy(j).start()
        if j == 0:
            near_copy.wait_recv()
            near_top = near[1][:, 0:1]
            chip_top = jnp.maximum(local_top, near_top)
            for i, own in enumerate((local_top, near_top)):
                spread = jnp.broadcast_to(jnp.exp(own - chip_top), (tokens, 128))
                for z in range(chips):
                    for half in range(2):
                        at = (2 * z + half) * rows
                        scale[i, half, z] = spread[at:at + rows, :]
        else:
            pass_on(j - 1)
    pass_on(parts - 1)

    remote(stats.at[pl.ds(0, n - 1)], stats.at[pl.ds(0, n - 1)], st_send, st_recv, partner).wait_recv()

    top = stats[0, 0:1, :]
    for k in range(1, n):
        top = jnp.maximum(top, stats[k, 0:1, :])
    total = jnp.zeros_like(top)
    picked = jnp.zeros_like(top)
    for k in range(n):
        total += stats[k, 1:2, :] * jnp.exp(stats[k, 0:1, :] - top)
        picked += stats[k, 2:3, :]
    loss_ref[...] = jnp.broadcast_to(jnp.sum(top + jnp.log(total) - picked, axis=1, keepdims=True) / tokens, loss_ref.shape)

    sub = lax.broadcasted_iota(jnp.int32, (128, tokens), 0)
    turned = jnp.where(sub == chips, jnp.exp(picked - top) / total - 1.0, jnp.where(sub == chips + 1, top, total))
    for z in range(chips):
        chip_top = jnp.maximum(stats[2 * z, 0:1, :], stats[2 * z + 1, 0:1, :])
        turned = jnp.where(sub == z, jnp.exp(chip_top - top) / total, turned)
    turned = jnp.transpose(turned)
    for k in range(n):
        mix[k] = turned[k * rows:(k + 1) * rows, :]
    factor = jnp.exp(local_top - turned[:, chips + 1:chips + 2]) / turned[:, chips + 2:chips + 3]
    hits = lax.broadcasted_iota(jnp.int32, (tokens, width), 1).astype(F32) == aim_ref[:, 0:1]
    g_ref[...] = (e_v[...] * factor - hits.astype(F32)).astype(BF16)

    for b in range(blocks):
        dw_ref[b * tall:(b + 1) * tall, :] = lax.dot_general(
            hid_ref[:, b * tall:(b + 1) * tall], g_ref[...], DOWN, preferred_element_type=F32
        ).astype(BF16)

    mine = mix[me]
    far = goal_far.at[pl.ds(0, chips - 1)]
    remote(far, far, far_send, far_recv, partner).wait_recv()
    there = rbuf.at[:, pl.ds(0, chips - 1)]
    remote(there, there, rs_send, rs_recv, partner).wait_recv()
    own_scale = mix[me]
    lanes = lax.broadcasted_iota(jnp.int32, (rows, 128), 1)
    own_scale = jnp.sum(jnp.where(lanes == chip, own_scale, 0.0), axis=1, keepdims=True)
    for j in range(parts):
        goals = goal_sum[chip, :, j * wide:(j + 1) * wide].astype(F32)
        summed = chip_sum(j, chip) * own_scale
        for k in range(1, chips):
            source = other(k)
            weight = jnp.sum(jnp.where(lanes == source, mine, 0.0), axis=1, keepdims=True)
            summed += rbuf[j, source].astype(F32) * weight
            goals += goal_far[source, :, j * wide:(j + 1) * wide].astype(F32)
        dh_ref[:, j * wide:(j + 1) * wide] = (summed + goals * mine[:, chips:chips + 1]).astype(BF16)

    for ref, sem in (
        (slots.at[:, 0, pl.ds(0, chips - 1)], ag_send), (slots.at[:, 0], fw_send), (stats.at[pl.ds(0, n - 1)], st_send),
        (near.at[0], near_send), (xbuf, x_send), (there, rs_send), (goal_in, goal_send), (far, far_send),
    ):
        remote(ref, ref, sem, st_recv, partner).wait_send()


def store_kernel(dw_v, dh_v, loss_v, dw_hbm, dh_hbm, loss_hbm, one_v, sem):
    one_v[...] = loss_v[0:1, 0:1]
    copies = []
    count = sem.shape[0] - 2
    tall = dw_v.shape[0] // count
    for b in range(count):
        at = pl.ds(b * tall, tall)
        copies.append(pltpu.make_async_copy(dw_v.at[at, :], dw_hbm.at[at, :], sem.at[2 + b]))
    copies.append(pltpu.make_async_copy(dh_v, dh_hbm, sem.at[0]))
    copies.append(pltpu.make_async_copy(one_v, loss_hbm, sem.at[1]))
    for copy in copies:
        copy.start()
    for copy in copies:
        copy.wait()


def body(n, hidden, weight, targets):
    rows, depth = hidden.shape
    width = weight.shape[1]
    tokens = rows * n
    chips = n // 2
    pieces = split(depth, 4, 256)
    parts = split(depth, 6, 256)
    span, wide = depth // pieces, depth // parts
    vmem = pl.BlockSpec(memory_space=pltpu.VMEM)
    dma = pltpu.SemaphoreType.DMA
    hbm = pl.BlockSpec(memory_space=pltpu.HBM)
    shared = (jax.ShapeDtypeStruct((depth, width), BF16), jax.ShapeDtypeStruct((rows, depth), BF16))
    tile = jax.ShapeDtypeStruct((8, 128), F32)
    held = pl.pallas_call(
        functools.partial(loss_kernel, n),
        out_shape=(*shared, tile),
        in_specs=[hbm, hbm, hbm],
        out_specs=(vmem, vmem, vmem),
        scratch_shapes=[
            pltpu.VMEM((1, tokens), jnp.int32),
            pltpu.VMEM((tokens, 128), F32),
            pltpu.VMEM((tokens, depth), BF16),
            pltpu.VMEM((tokens, width), BF16),
            pltpu.VMEM((depth, width), BF16),
            pltpu.VMEM((pieces, 2, chips, rows, span), BF16),
            pltpu.VMEM((tokens, width), F32),
            pltpu.VMEM((n, 8, tokens), F32),
            pltpu.VMEM((2, tokens, 128), F32),
            pltpu.VMEM((2, 2, chips, rows, 128), F32),
            pltpu.VMEM((n, rows, 128), F32),
            pltpu.VMEM((parts, 2, chips, rows, wide), F32),
            pltpu.VMEM((parts, chips, rows, wide), F32),
            pltpu.VMEM((parts, chips, rows, wide), BF16),
            pltpu.VMEM((parts, chips, rows, wide), BF16),
            pltpu.VMEM((2, chips, rows, depth), BF16),
            pltpu.VMEM((chips, rows, depth), BF16),
            pltpu.VMEM((chips, rows, depth), BF16),
            pltpu.VMEM((chips, rows, depth), BF16),
            dma((pieces + 1,)),
            dma((pieces,)),
            dma((8,)),
            dma((pieces,)),
            dma((pieces,)),
            dma((5,)),
            dma((parts,)),
        ],
        compiler_params=pltpu.CompilerParams(
            collective_id=0, has_side_effects=True, vmem_limit_bytes=45 * 1024 * 1024
        ),
    )(*[pltpu.with_memory_space_constraint(x, pltpu.HBM) for x in (hidden, weight, targets.reshape(1, tokens))])
    d_weight, d_hidden, loss = pl.pallas_call(
        store_kernel,
        out_shape=(*shared, jax.ShapeDtypeStruct((1, 1), F32)),
        in_specs=[vmem, vmem, vmem],
        out_specs=(hbm, hbm, hbm),
        scratch_shapes=[pltpu.VMEM((1, 1), F32), dma((2 + split(depth, 12, 16),))],
        compiler_params=pltpu.CompilerParams(vmem_limit_bytes=2 * 1024 * 1024),
    )(*held)
    return loss.reshape(1), d_hidden, d_weight


def solution(mesh):
    placed = (P(("dp", "vocab"), None), P(None, "vocab"), P("dp"))
    return jax.shard_map(
        functools.partial(body, mesh.shape["vocab"]),
        mesh=mesh,
        in_specs=placed,
        out_specs=(P("dp"), P(("dp", "vocab"), None), P("dp", "vocab")),
        check_vma=False,
    )
```

```python
import functools

import jax
import jax.numpy as jnp
from jax import lax
from jax.experimental import pallas as pl
from jax.experimental.pallas import tpu as pltpu
from jax.sharding import PartitionSpec as P

MESH = pl.DeviceIdType.MESH
F32 = jnp.float32
BF16 = jnp.bfloat16
ACROSS = (((1,), (1,)), ((), ()))
DOWN = (((0,), (0,)), ((), ()))


def split(length, most, unit):
    for parts in range(most, 0, -1):
        if length % (parts * unit) == 0:
            return parts
    return 1


def plan(units):
    if units == 12:
        return [6, 6], 1, [[], [0, 1]]
    return [1] * units, 1, [[] if j == 0 else [j - 1] for j in range(units - 1)] + [[units - 2, units - 1] if units > 1 else [0]]


def remote(src, dst, send, recv, device):
    return pltpu.make_async_remote_copy(
        src_ref=src, dst_ref=dst, send_sem=send, recv_sem=recv, device_id={"vocab": device}, device_id_type=MESH
    )


def loss_kernel(
    n, widths, turn, after, h_hbm, w_hbm, t_hbm, dw_ref, dh_ref, loss_ref,
    t_ref, aim_ref, hid_ref, g_ref, w_v, slots, e_v, stats, near, scale, mix, part, xbuf, outb, rbuf,
    goal, goal_in, goal_sum, goal_far,
    in_sem, w_sem, send_sem, ag_recv, fw_recv, recv_sem, x_recv,
):
    me = lax.axis_index("vocab")
    chips = n // 2
    chip, core = me // 2, me % 2
    partner = chip * 2 + (1 - core)
    pieces, rows, span = slots.shape[0], slots.shape[3], slots.shape[4]
    tokens, width = e_v.shape
    depth = w_v.shape[0]
    blocks = split(depth, 6, 256)
    tall = depth // blocks
    starts = [sum(widths[:j]) for j in range(len(widths))]
    ag_send, fw_send, st_send, near_send, x_send, rs_send, goal_send, far_send = [send_sem.at[i] for i in range(8)]
    st_recv, near_recv, rs_recv, goal_recv, far_recv = [recv_sem.at[i] for i in range(5)]

    above = chips - 1 - chip

    def other(k):
        up = (above - k + chips) // chips
        return up * (chips - k) + (1 - up) * (k - 1 - above)

    takes = [
        pltpu.make_async_copy(h_hbm.at[:, pl.ds(a * span, span)], slots.at[a, core, chip], in_sem.at[a])
        for a in range(pieces)
    ]
    takes.append(pltpu.make_async_copy(t_hbm, t_ref, in_sem.at[pieces]))
    for take in takes:
        take.start()
    loads = [
        pltpu.make_async_copy(w_hbm.at[pl.ds(a * span, span), :], w_v.at[pl.ds(a * span, span), :], w_sem.at[a])
        for a in range(pieces)
    ]

    barrier = pltpu.get_barrier_semaphore()
    for k in range(1, n):
        pl.semaphore_signal(barrier, inc=1, device_id={"vocab": lax.rem(me + k, n)}, device_id_type=MESH)
    for take in takes:
        take.wait()
    for load in loads:
        load.start()
    aim_ref[...] = jnp.transpose(jnp.broadcast_to((t_ref[...] - me * width).astype(F32), (128, tokens)))
    pl.semaphore_wait(barrier, n - 1)

    for a in range(pieces):
        own = slots.at[a, core, chip]
        for k in range(1, chips):
            remote(own, own, ag_send, ag_recv.at[a], other(k) * 2 + core).start()

    hits = lax.broadcasted_iota(jnp.int32, (tokens, width), 1).astype(F32) == aim_ref[:, 0:1]
    g_ref[...] = hits.astype(F32).astype(BF16)
    for load in loads:
        load.wait()
    for b in range(blocks):
        term = lax.dot_general(g_ref[...], w_v[b * tall:(b + 1) * tall, :], ACROSS, preferred_element_type=F32)
        for z in range(chips):
            for half in range(2):
                at = (2 * z + half) * rows
                goal[half, z, :, b * tall:(b + 1) * tall] = term[at:at + rows, :].astype(BF16)
    goal_copy = remote(goal.at[1 - core], goal_in, goal_send, goal_recv, partner)
    goal_copy.start()
    goal_copy.wait_recv()
    for z in range(chips):
        goal_sum[z] = (goal[core, z].astype(F32) + goal_in[z].astype(F32)).astype(BF16)
    for k in range(1, chips):
        remote(goal_sum.at[other(k)], goal_far.at[chip], far_send, far_recv, other(k) * 2 + core).start()

    def finish(a):
        remote(slots.at[a, 1 - core], slots.at[a, 1 - core], fw_send, fw_recv.at[a], partner).wait_recv()
        for z in range(chips):
            both = jnp.concatenate([slots[a, 0, z].astype(F32), slots[a, 1, z].astype(F32)], axis=0)
            hid_ref[2 * rows * z:2 * rows * (z + 1), a * span:(a + 1) * span] = both.astype(BF16)
        term = jnp.dot(
            hid_ref[:, a * span:(a + 1) * span], w_v[a * span:(a + 1) * span, :], preferred_element_type=F32
        )
        if a == 0:
            e_v[...] = term
        else:
            e_v[...] += term

    for a in range(pieces):
        there = slots.at[a, core, pl.ds(0, chips - 1)]
        remote(there, there, ag_send, ag_recv.at[a], partner).wait_recv()
        remote(slots.at[a, core], slots.at[a, core], fw_send, fw_recv.at[a], partner).start()
        if a > 0:
            finish(a - 1)
    finish(pieces - 1)

    logits = e_v[...]
    hits = lax.broadcasted_iota(jnp.int32, (tokens, width), 1).astype(F32) == aim_ref[:, 0:1]
    local_top = jnp.max(logits, axis=1, keepdims=True)
    expo = jnp.exp(logits - local_top)
    e_v[...] = expo
    g_ref[...] = jnp.where(hits, 0.0, expo).astype(BF16)
    local_total = jnp.sum(expo, axis=1, keepdims=True)
    local_picked = jnp.sum(jnp.where(hits, logits, 0.0), axis=1, keepdims=True)
    lane = lax.broadcasted_iota(jnp.int32, (tokens, 128), 1)
    packed = jnp.where(lane == 0, local_top, jnp.where(lane == 1, local_total, local_picked))
    near[0] = packed
    near_copy = remote(near.at[0], near.at[1], near_send, near_recv, partner)
    near_copy.start()
    stats[me] = jnp.transpose(packed)[0:8, :]
    for k in range(1, n):
        remote(stats.at[me], stats.at[me], st_send, st_recv, lax.rem(me + k, n)).start()

    def pair_copy(j):
        at = pl.ds(starts[j], widths[j])
        return remote(part.at[1 - core, :, :, at], xbuf.at[:, :, at], x_send, x_recv.at[j], partner)

    def chip_sum(z, at):
        return part[core, z, :, at] * scale[0, core, z][:, 0:1] + xbuf[z, :, at] * scale[1, core, z][:, 0:1]

    def pass_on(j):
        at = slice(starts[j], starts[j] + widths[j])
        pair_copy(j).wait_recv()
        for z in range(chips):
            outb[z, :, at] = chip_sum(z, at).astype(BF16)
        at = pl.ds(starts[j], widths[j])
        for k in range(1, chips):
            remote(outb.at[other(k), :, at], rbuf.at[chip, :, at], rs_send, rs_recv, other(k) * 2 + core).start()

    for j in range(len(widths)):
        if j == turn:
            near_copy.wait_recv()
            near_top = near[1][:, 0:1]
            chip_top = jnp.maximum(local_top, near_top)
            for i, own in enumerate((local_top, near_top)):
                spread = jnp.broadcast_to(jnp.exp(own - chip_top), (tokens, 128))
                for z in range(chips):
                    for half in range(2):
                        at = (2 * z + half) * rows
                        scale[i, half, z] = spread[at:at + rows, :]
        term = lax.dot_general(
            g_ref[...], w_v[starts[j]:starts[j] + widths[j], :], ACROSS, preferred_element_type=F32
        )
        for z in range(chips):
            for half in range(2):
                at = (2 * z + half) * rows
                part[half, z, :, starts[j]:starts[j] + widths[j]] = term[at:at + rows, :]
        pair_copy(j).start()
        for i in after[j]:
            pass_on(i)

    remote(stats.at[pl.ds(0, n - 1)], stats.at[pl.ds(0, n - 1)], st_send, st_recv, partner).wait_recv()

    top = stats[0, 0:1, :]
    for k in range(1, n):
        top = jnp.maximum(top, stats[k, 0:1, :])
    total = jnp.zeros_like(top)
    picked = jnp.zeros_like(top)
    for k in range(n):
        total += stats[k, 1:2, :] * jnp.exp(stats[k, 0:1, :] - top)
        picked += stats[k, 2:3, :]
    loss_ref[...] = jnp.broadcast_to(jnp.sum(top + jnp.log(total) - picked, axis=1, keepdims=True) / tokens, loss_ref.shape)

    sub = lax.broadcasted_iota(jnp.int32, (128, tokens), 0)
    turned = jnp.where(sub == chips, jnp.exp(picked - top) / total - 1.0, jnp.where(sub == chips + 1, top, total))
    for z in range(chips):
        chip_top = jnp.maximum(stats[2 * z, 0:1, :], stats[2 * z + 1, 0:1, :])
        turned = jnp.where(sub == z, jnp.exp(chip_top - top) / total, turned)
    turned = jnp.transpose(turned)
    for k in range(n):
        mix[k] = turned[k * rows:(k + 1) * rows, :]
    factor = jnp.exp(local_top - turned[:, chips + 1:chips + 2]) / turned[:, chips + 2:chips + 3]
    hits = lax.broadcasted_iota(jnp.int32, (tokens, width), 1).astype(F32) == aim_ref[:, 0:1]
    g_ref[...] = (e_v[...] * factor - hits.astype(F32)).astype(BF16)

    for b in range(blocks):
        dw_ref[b * tall:(b + 1) * tall, :] = lax.dot_general(
            hid_ref[:, b * tall:(b + 1) * tall], g_ref[...], DOWN, preferred_element_type=F32
        ).astype(BF16)

    mine = mix[me]
    far = goal_far.at[pl.ds(0, chips - 1)]
    remote(far, far, far_send, far_recv, partner).wait_recv()
    there = rbuf.at[pl.ds(0, chips - 1)]
    remote(there, there, rs_send, rs_recv, partner).wait_recv()
    lanes = lax.broadcasted_iota(jnp.int32, (rows, 128), 1)
    share = [
        jnp.sum(jnp.where(lanes == z, mine, 0.0), axis=1, keepdims=True)
        for z in [chip] + [other(k) for k in range(1, chips)]
    ]
    for b in range(blocks):
        at = slice(b * tall, (b + 1) * tall)
        goals = goal_sum[chip, :, at].astype(F32)
        summed = chip_sum(chip, at) * share[0]
        for k in range(1, chips):
            summed += rbuf[other(k), :, at].astype(F32) * share[k]
            goals += goal_far[other(k), :, at].astype(F32)
        dh_ref[:, at] = (summed + goals * mine[:, chips:chips + 1]).astype(BF16)

    for ref, sem in (
        (slots.at[:, 0, pl.ds(0, chips - 1)], ag_send), (slots.at[:, 0], fw_send), (stats.at[pl.ds(0, n - 1)], st_send),
        (near.at[0], near_send), (xbuf, x_send), (there, rs_send), (goal_in, goal_send), (far, far_send),
    ):
        remote(ref, ref, sem, st_recv, partner).wait_send()


def store_kernel(dw_v, dh_v, loss_v, dw_hbm, dh_hbm, loss_hbm, one_v, sem):
    one_v[...] = loss_v[0:1, 0:1]
    copies = []
    count = sem.shape[0] - 2
    tall = dw_v.shape[0] // count
    for b in range(count):
        at = pl.ds(b * tall, tall)
        copies.append(pltpu.make_async_copy(dw_v.at[at, :], dw_hbm.at[at, :], sem.at[2 + b]))
    copies.append(pltpu.make_async_copy(dh_v, dh_hbm, sem.at[0]))
    copies.append(pltpu.make_async_copy(one_v, loss_hbm, sem.at[1]))
    for copy in copies:
        copy.start()
    for copy in copies:
        copy.wait()


def body(n, hidden, weight, targets):
    rows, depth = hidden.shape
    width = weight.shape[1]
    tokens = rows * n
    chips = n // 2
    pieces = split(depth, 3, 256)
    unit = depth // split(depth, 12, 128)
    widths, turn, after = plan(depth // unit)
    widths = [w * unit for w in widths]
    span = depth // pieces
    vmem = pl.BlockSpec(memory_space=pltpu.VMEM)
    dma = pltpu.SemaphoreType.DMA
    hbm = pl.BlockSpec(memory_space=pltpu.HBM)
    shared = (jax.ShapeDtypeStruct((depth, width), BF16), jax.ShapeDtypeStruct((rows, depth), BF16))
    tile = jax.ShapeDtypeStruct((8, 128), F32)
    held = pl.pallas_call(
        functools.partial(loss_kernel, n, widths, turn, after),
        out_shape=(*shared, tile),
        in_specs=[hbm, hbm, hbm],
        out_specs=(vmem, vmem, vmem),
        scratch_shapes=[
            pltpu.VMEM((1, tokens), jnp.int32),
            pltpu.VMEM((tokens, 128), F32),
            pltpu.VMEM((tokens, depth), BF16),
            pltpu.VMEM((tokens, width), BF16),
            pltpu.VMEM((depth, width), BF16),
            pltpu.VMEM((pieces, 2, chips, rows, span), BF16),
            pltpu.VMEM((tokens, width), F32),
            pltpu.VMEM((n, 8, tokens), F32),
            pltpu.VMEM((2, tokens, 128), F32),
            pltpu.VMEM((2, 2, chips, rows, 128), F32),
            pltpu.VMEM((n, rows, 128), F32),
            pltpu.VMEM((2, chips, rows, depth), F32),
            pltpu.VMEM((chips, rows, depth), F32),
            pltpu.VMEM((chips, rows, depth), BF16),
            pltpu.VMEM((chips, rows, depth), BF16),
            pltpu.VMEM((2, chips, rows, depth), BF16),
            pltpu.VMEM((chips, rows, depth), BF16),
            pltpu.VMEM((chips, rows, depth), BF16),
            pltpu.VMEM((chips, rows, depth), BF16),
            dma((pieces + 1,)),
            dma((pieces,)),
            dma((8,)),
            dma((pieces,)),
            dma((pieces,)),
            dma((5,)),
            dma((len(widths),)),
        ],
        compiler_params=pltpu.CompilerParams(
            collective_id=0, has_side_effects=True, vmem_limit_bytes=45 * 1024 * 1024
        ),
    )(*[pltpu.with_memory_space_constraint(x, pltpu.HBM) for x in (hidden, weight, targets.reshape(1, tokens))])
    d_weight, d_hidden, loss = pl.pallas_call(
        store_kernel,
        out_shape=(*shared, jax.ShapeDtypeStruct((1, 1), F32)),
        in_specs=[vmem, vmem, vmem],
        out_specs=(hbm, hbm, hbm),
        scratch_shapes=[pltpu.VMEM((1, 1), F32), dma((2 + split(depth, 12, 16),))],
        compiler_params=pltpu.CompilerParams(vmem_limit_bytes=2 * 1024 * 1024),
    )(*held)
    return loss.reshape(1), d_hidden, d_weight


def solution(mesh):
    placed = (P(("dp", "vocab"), None), P(None, "vocab"), P("dp"))
    return jax.shard_map(
        functools.partial(body, mesh.shape["vocab"]),
        mesh=mesh,
        in_specs=placed,
        out_specs=(P("dp"), P(("dp", "vocab"), None), P("dp", "vocab")),
        check_vma=False,
    )
```

```python
import functools

import jax
import jax.numpy as jnp
from jax import lax
from jax.experimental import pallas as pl
from jax.experimental.pallas import tpu as pltpu
from jax.sharding import PartitionSpec as P

MESH = pl.DeviceIdType.MESH
F32 = jnp.float32
BF16 = jnp.bfloat16
ACROSS = (((1,), (1,)), ((), ()))
DOWN = (((0,), (0,)), ((), ()))


def split(length, most, unit):
    for parts in range(most, 0, -1):
        if length % (parts * unit) == 0:
            return parts
    return 1


def plan(units):
    if units == 12:
        return [6, 6], 1, [[], [0, 1]]
    return [1] * units, 1, [[] if j == 0 else [j - 1] for j in range(units - 1)] + [[units - 2, units - 1] if units > 1 else [0]]


def remote(src, dst, send, recv, device):
    return pltpu.make_async_remote_copy(
        src_ref=src, dst_ref=dst, send_sem=send, recv_sem=recv, device_id={"vocab": device}, device_id_type=MESH
    )


def loss_kernel(
    n, widths, turn, after, h_hbm, w_hbm, t_hbm, dw_ref, dh_ref, loss_ref,
    t_ref, aim_ref, hid_ref, g_ref, w_v, slots, e_v, stats, near, scale, mix, part, xbuf, outb, rbuf,
    goal, goal_in, goal_sum, goal_far,
    in_sem, w_sem, send_sem, ag_recv, fw_recv, recv_sem, x_recv,
):
    me = lax.axis_index("vocab")
    chips = n // 2
    chip, core = me // 2, me % 2
    away = 1 - core
    partner = chip * 2 + away
    pieces, rows, span = slots.shape[0], slots.shape[3], slots.shape[4]
    tokens, width = e_v.shape
    depth = w_v.shape[0]
    blocks = split(depth, 6, 256)
    tall = depth // blocks
    starts = [sum(widths[:j]) for j in range(len(widths))]
    ag_send, fw_send, st_send, near_send, x_send, rs_send, goal_send, far_send = [send_sem.at[i] for i in range(8)]
    st_recv, near_recv, rs_recv, goal_recv, far_recv = [recv_sem.at[i] for i in range(5)]

    above = chips - 1 - chip

    def other(k):
        up = (above - k + chips) // chips
        return up * (chips - k) + (1 - up) * (k - 1 - above)

    takes = [
        pltpu.make_async_copy(h_hbm.at[:, pl.ds(a * span, span)], slots.at[a, core, chip], in_sem.at[a])
        for a in range(pieces)
    ]
    takes.append(pltpu.make_async_copy(t_hbm, t_ref, in_sem.at[pieces]))
    for take in takes:
        take.start()
    loads = [
        pltpu.make_async_copy(w_hbm.at[pl.ds(a * span, span), :], w_v.at[pl.ds(a * span, span), :], w_sem.at[a])
        for a in range(pieces)
    ]

    barrier = pltpu.get_barrier_semaphore()
    for k in range(1, n):
        pl.semaphore_signal(barrier, inc=1, device_id={"vocab": lax.rem(me + k, n)}, device_id_type=MESH)
    for take in takes:
        take.wait()
    for load in loads:
        load.start()
    aim_ref[...] = jnp.transpose(jnp.broadcast_to((t_ref[...] - me * width).astype(F32), (128, tokens)))
    pl.semaphore_wait(barrier, n - 1)

    for a in range(pieces):
        own = slots.at[a, core, chip]
        for k in range(1, chips):
            remote(own, own, ag_send, ag_recv.at[a], other(k) * 2 + away).start()
        remote(own, own, ag_send, fw_recv.at[a], partner).start()

    hits = lax.broadcasted_iota(jnp.int32, (tokens, width), 1).astype(F32) == aim_ref[:, 0:1]
    g_ref[...] = hits.astype(F32).astype(BF16)
    for load in loads:
        load.wait()
    for b in range(blocks):
        term = lax.dot_general(g_ref[...], w_v[b * tall:(b + 1) * tall, :], ACROSS, preferred_element_type=F32)
        for z in range(chips):
            for half in range(2):
                at = (2 * z + half) * rows
                goal[half, z, :, b * tall:(b + 1) * tall] = term[at:at + rows, :].astype(BF16)
    goal_copy = remote(goal.at[core], goal_in, goal_send, goal_recv, partner)
    goal_copy.start()
    goal_copy.wait_recv()
    for z in range(chips):
        goal_sum[z] = (goal[away, z].astype(F32) + goal_in[z].astype(F32)).astype(BF16)
    for k in range(1, chips):
        remote(goal_sum.at[other(k)], goal_far.at[chip], far_send, far_recv, other(k) * 2 + away).start()
    remote(goal_sum.at[chip], goal_far.at[chip], far_send, far_recv, partner).start()

    def finish(a):
        remote(slots.at[a, core], slots.at[a, core], fw_send, fw_recv.at[a], partner).wait_recv()
        for z in range(chips):
            both = jnp.concatenate([slots[a, 0, z].astype(F32), slots[a, 1, z].astype(F32)], axis=0)
            hid_ref[2 * rows * z:2 * rows * (z + 1), a * span:(a + 1) * span] = both.astype(BF16)
        term = jnp.dot(
            hid_ref[:, a * span:(a + 1) * span], w_v[a * span:(a + 1) * span, :], preferred_element_type=F32
        )
        if a == 0:
            e_v[...] = term
        else:
            e_v[...] += term

    for a in range(pieces):
        there = slots.at[a, away, pl.ds(0, chips - 1)]
        remote(there, there, ag_send, ag_recv.at[a], partner).wait_recv()
        for k in range(1, chips):
            there = slots.at[a, away, other(k)]
            remote(there, there, fw_send, fw_recv.at[a], partner).start()
        if a > 0:
            finish(a - 1)
    finish(pieces - 1)

    logits = e_v[...]
    hits = lax.broadcasted_iota(jnp.int32, (tokens, width), 1).astype(F32) == aim_ref[:, 0:1]
    local_top = jnp.max(logits, axis=1, keepdims=True)
    expo = jnp.exp(logits - local_top)
    e_v[...] = expo
    g_ref[...] = jnp.where(hits, 0.0, expo).astype(BF16)
    local_total = jnp.sum(expo, axis=1, keepdims=True)
    local_picked = jnp.sum(jnp.where(hits, logits, 0.0), axis=1, keepdims=True)
    lane = lax.broadcasted_iota(jnp.int32, (tokens, 128), 1)
    packed = jnp.where(lane == 0, local_top, jnp.where(lane == 1, local_total, local_picked))
    near[0] = packed
    near_copy = remote(near.at[0], near.at[1], near_send, near_recv, partner)
    near_copy.start()
    stats[me] = jnp.transpose(packed)[0:8, :]
    for k in range(1, n):
        remote(stats.at[me], stats.at[me], st_send, st_recv, lax.rem(me + k, n)).start()

    def pair_copy(j):
        at = pl.ds(starts[j], widths[j])
        return remote(part.at[core, :, :, at], xbuf.at[:, :, at], x_send, x_recv.at[j], partner)

    def chip_sum(z, at):
        return part[away, z, :, at] * scale[0, away, z][:, 0:1] + xbuf[z, :, at] * scale[1, away, z][:, 0:1]

    def pass_on(j):
        at = slice(starts[j], starts[j] + widths[j])
        pair_copy(j).wait_recv()
        for z in range(chips):
            outb[z, :, at] = chip_sum(z, at).astype(BF16)
        at = pl.ds(starts[j], widths[j])
        for k in range(1, chips):
            remote(outb.at[other(k), :, at], rbuf.at[chip, :, at], rs_send, rs_recv, other(k) * 2 + away).start()
        remote(outb.at[chip, :, at], rbuf.at[chip, :, at], rs_send, rs_recv, partner).start()

    for j in range(len(widths)):
        if j == turn:
            near_copy.wait_recv()
            near_top = near[1][:, 0:1]
            chip_top = jnp.maximum(local_top, near_top)
            for i, own in enumerate((local_top, near_top)):
                spread = jnp.broadcast_to(jnp.exp(own - chip_top), (tokens, 128))
                for z in range(chips):
                    for half in range(2):
                        at = (2 * z + half) * rows
                        scale[i, half, z] = spread[at:at + rows, :]
        term = lax.dot_general(
            g_ref[...], w_v[starts[j]:starts[j] + widths[j], :], ACROSS, preferred_element_type=F32
        )
        for z in range(chips):
            for half in range(2):
                at = (2 * z + half) * rows
                part[half, z, :, starts[j]:starts[j] + widths[j]] = term[at:at + rows, :]
        pair_copy(j).start()
        for i in after[j]:
            pass_on(i)

    remote(stats.at[pl.ds(0, n - 1)], stats.at[pl.ds(0, n - 1)], st_send, st_recv, partner).wait_recv()

    top = stats[0, 0:1, :]
    for k in range(1, n):
        top = jnp.maximum(top, stats[k, 0:1, :])
    total = jnp.zeros_like(top)
    picked = jnp.zeros_like(top)
    for k in range(n):
        total += stats[k, 1:2, :] * jnp.exp(stats[k, 0:1, :] - top)
        picked += stats[k, 2:3, :]
    loss_ref[...] = jnp.broadcast_to(jnp.sum(top + jnp.log(total) - picked, axis=1, keepdims=True) / tokens, loss_ref.shape)

    sub = lax.broadcasted_iota(jnp.int32, (128, tokens), 0)
    turned = jnp.where(sub == chips, jnp.exp(picked - top) / total - 1.0, jnp.where(sub == chips + 1, top, total))
    for z in range(chips):
        chip_top = jnp.maximum(stats[2 * z, 0:1, :], stats[2 * z + 1, 0:1, :])
        turned = jnp.where(sub == z, jnp.exp(chip_top - top) / total, turned)
    turned = jnp.transpose(turned)
    for k in range(n):
        mix[k] = turned[k * rows:(k + 1) * rows, :]
    factor = jnp.exp(local_top - turned[:, chips + 1:chips + 2]) / turned[:, chips + 2:chips + 3]
    hits = lax.broadcasted_iota(jnp.int32, (tokens, width), 1).astype(F32) == aim_ref[:, 0:1]
    g_ref[...] = (e_v[...] * factor - hits.astype(F32)).astype(BF16)

    for b in range(blocks):
        dw_ref[b * tall:(b + 1) * tall, :] = lax.dot_general(
            hid_ref[:, b * tall:(b + 1) * tall], g_ref[...], DOWN, preferred_element_type=F32
        ).astype(BF16)

    mine = mix[me]
    remote(goal_far, goal_far, far_send, far_recv, partner).wait_recv()
    remote(rbuf, rbuf, rs_send, rs_recv, partner).wait_recv()
    for b in range(blocks):
        at = slice(b * tall, (b + 1) * tall)
        goals = jnp.zeros((rows, tall), F32)
        summed = jnp.zeros((rows, tall), F32)
        for z in range(chips):
            summed += rbuf[z, :, at].astype(F32) * mine[:, z:z + 1]
            goals += goal_far[z, :, at].astype(F32)
        dh_ref[:, at] = (summed + goals * mine[:, chips:chips + 1]).astype(BF16)

    for ref, sem in (
        (slots.at[:, 0], ag_send), (slots.at[:, 0, pl.ds(0, chips - 1)], fw_send), (stats.at[pl.ds(0, n - 1)], st_send),
        (near.at[0], near_send), (xbuf, x_send), (rbuf, rs_send), (goal_in, goal_send), (goal_far, far_send),
    ):
        remote(ref, ref, sem, st_recv, partner).wait_send()


def store_kernel(dw_v, dh_v, loss_v, dw_hbm, dh_hbm, loss_hbm, one_v, sem):
    one_v[...] = loss_v[0:1, 0:1]
    copies = []
    count = sem.shape[0] - 2
    tall = dw_v.shape[0] // count
    for b in range(count):
        at = pl.ds(b * tall, tall)
        copies.append(pltpu.make_async_copy(dw_v.at[at, :], dw_hbm.at[at, :], sem.at[2 + b]))
    copies.append(pltpu.make_async_copy(dh_v, dh_hbm, sem.at[0]))
    copies.append(pltpu.make_async_copy(one_v, loss_hbm, sem.at[1]))
    for copy in copies:
        copy.start()
    for copy in copies:
        copy.wait()


def body(n, hidden, weight, targets):
    rows, depth = hidden.shape
    width = weight.shape[1]
    tokens = rows * n
    chips = n // 2
    pieces = split(depth, 3, 256)
    unit = depth // split(depth, 12, 128)
    widths, turn, after = plan(depth // unit)
    widths = [w * unit for w in widths]
    span = depth // pieces
    vmem = pl.BlockSpec(memory_space=pltpu.VMEM)
    dma = pltpu.SemaphoreType.DMA
    hbm = pl.BlockSpec(memory_space=pltpu.HBM)
    shared = (jax.ShapeDtypeStruct((depth, width), BF16), jax.ShapeDtypeStruct((rows, depth), BF16))
    tile = jax.ShapeDtypeStruct((8, 128), F32)
    held = pl.pallas_call(
        functools.partial(loss_kernel, n, widths, turn, after),
        out_shape=(*shared, tile),
        in_specs=[hbm, hbm, hbm],
        out_specs=(vmem, vmem, vmem),
        scratch_shapes=[
            pltpu.VMEM((1, tokens), jnp.int32),
            pltpu.VMEM((tokens, 128), F32),
            pltpu.VMEM((tokens, depth), BF16),
            pltpu.VMEM((tokens, width), BF16),
            pltpu.VMEM((depth, width), BF16),
            pltpu.VMEM((pieces, 2, chips, rows, span), BF16),
            pltpu.VMEM((tokens, width), F32),
            pltpu.VMEM((n, 8, tokens), F32),
            pltpu.VMEM((2, tokens, 128), F32),
            pltpu.VMEM((2, 2, chips, rows, 128), F32),
            pltpu.VMEM((n, rows, 128), F32),
            pltpu.VMEM((2, chips, rows, depth), F32),
            pltpu.VMEM((chips, rows, depth), F32),
            pltpu.VMEM((chips, rows, depth), BF16),
            pltpu.VMEM((chips, rows, depth), BF16),
            pltpu.VMEM((2, chips, rows, depth), BF16),
            pltpu.VMEM((chips, rows, depth), BF16),
            pltpu.VMEM((chips, rows, depth), BF16),
            pltpu.VMEM((chips, rows, depth), BF16),
            dma((pieces + 1,)),
            dma((pieces,)),
            dma((8,)),
            dma((pieces,)),
            dma((pieces,)),
            dma((5,)),
            dma((len(widths),)),
        ],
        compiler_params=pltpu.CompilerParams(
            collective_id=0, has_side_effects=True, vmem_limit_bytes=45 * 1024 * 1024
        ),
    )(*[pltpu.with_memory_space_constraint(x, pltpu.HBM) for x in (hidden, weight, targets.reshape(1, tokens))])
    d_weight, d_hidden, loss = pl.pallas_call(
        store_kernel,
        out_shape=(*shared, jax.ShapeDtypeStruct((1, 1), F32)),
        in_specs=[vmem, vmem, vmem],
        out_specs=(hbm, hbm, hbm),
        scratch_shapes=[pltpu.VMEM((1, 1), F32), dma((2 + split(depth, 12, 16),))],
        compiler_params=pltpu.CompilerParams(vmem_limit_bytes=2 * 1024 * 1024),
    )(*held)
    return loss.reshape(1), d_hidden, d_weight


def solution(mesh):
    placed = (P(("dp", "vocab"), None), P(None, "vocab"), P("dp"))
    return jax.shard_map(
        functools.partial(body, mesh.shape["vocab"]),
        mesh=mesh,
        in_specs=placed,
        out_specs=(P("dp"), P(("dp", "vocab"), None), P("dp", "vocab")),
        check_vma=False,
    )
```

```python
import functools

import jax
import jax.numpy as jnp
from jax import lax
from jax.experimental import pallas as pl
from jax.experimental.pallas import tpu as pltpu
from jax.sharding import PartitionSpec as P

MESH = pl.DeviceIdType.MESH
F32 = jnp.float32
BF16 = jnp.bfloat16
DOWN = (((0,), (0,)), ((), ()))


def split(length, most, unit):
    for parts in range(most, 0, -1):
        if length % (parts * unit) == 0:
            return parts
    return 1


def plan(units):
    if units == 12:
        return [4, 4, 4], 2, [[], [], [0, 1, 2]]
    return [1] * units, 1, [[] if j == 0 else [j - 1] for j in range(units - 1)] + [[units - 2, units - 1] if units > 1 else [0]]


def remote(src, dst, send, recv, device):
    return pltpu.make_async_remote_copy(
        src_ref=src, dst_ref=dst, send_sem=send, recv_sem=recv, device_id={"vocab": device}, device_id_type=MESH
    )


def loss_kernel(
    n, widths, turn, after, h_hbm, w_hbm, t_hbm, dw_ref, dh_ref, loss_ref,
    t_ref, aim_ref, hid_ref, g_ref, w_v, turned_v, slots, e_v, stats, near, scale, mix, part, xbuf, outb, rbuf,
    goal, goal_in, goal_sum, goal_far,
    in_sem, w_sem, send_sem, ag_recv, fw_recv, recv_sem, x_recv,
):
    me = lax.axis_index("vocab")
    chips = n // 2
    chip, core = me // 2, me % 2
    away = 1 - core
    partner = chip * 2 + away
    pieces, rows, span = slots.shape[0], slots.shape[3], slots.shape[4]
    tokens, width = e_v.shape
    depth = w_v.shape[0]
    blocks = split(depth, 6, 256)
    tall = depth // blocks
    starts = [sum(widths[:j]) for j in range(len(widths))]
    ag_send, fw_send, st_send, near_send, x_send, rs_send, goal_send, far_send = [send_sem.at[i] for i in range(8)]
    st_recv, near_recv, rs_recv, goal_recv, far_recv = [recv_sem.at[i] for i in range(5)]

    above = chips - 1 - chip

    def other(k):
        up = (above - k + chips) // chips
        return up * (chips - k) + (1 - up) * (k - 1 - above)

    takes = [
        pltpu.make_async_copy(h_hbm.at[:, pl.ds(a * span, span)], slots.at[a, core, chip], in_sem.at[a])
        for a in range(pieces)
    ]
    takes.append(pltpu.make_async_copy(t_hbm, t_ref, in_sem.at[pieces]))
    for take in takes:
        take.start()
    loads = [
        pltpu.make_async_copy(w_hbm.at[pl.ds(a * span, span), :], w_v.at[pl.ds(a * span, span), :], w_sem.at[a])
        for a in range(pieces)
    ]

    barrier = pltpu.get_barrier_semaphore()
    for k in range(1, n):
        pl.semaphore_signal(barrier, inc=1, device_id={"vocab": lax.rem(me + k, n)}, device_id_type=MESH)
    for take in takes:
        take.wait()
    for load in loads:
        load.start()
    aim_ref[...] = jnp.transpose(jnp.broadcast_to((t_ref[...] - me * width).astype(F32), (128, tokens)))
    pl.semaphore_wait(barrier, n - 1)

    for a in range(pieces):
        own = slots.at[a, core, chip]
        for k in range(1, chips):
            remote(own, own, ag_send, ag_recv.at[a], other(k) * 2 + away).start()
        remote(own, own, ag_send, fw_recv.at[a], partner).start()

    hits = lax.broadcasted_iota(jnp.int32, (tokens, width), 1).astype(F32) == aim_ref[:, 0:1]
    g_ref[...] = hits.astype(F32).astype(BF16)
    for load in loads:
        load.wait()
    for b in range(blocks):
        turned_v[:, b * tall:(b + 1) * tall] = jnp.transpose(w_v[b * tall:(b + 1) * tall, :])
        term = jnp.dot(g_ref[...], turned_v[:, b * tall:(b + 1) * tall], preferred_element_type=F32)
        for z in range(chips):
            for half in range(2):
                at = (2 * z + half) * rows
                goal[half, z, :, b * tall:(b + 1) * tall] = term[at:at + rows, :].astype(BF16)
    goal_copy = remote(goal.at[core], goal_in, goal_send, goal_recv, partner)
    goal_copy.start()
    goal_copy.wait_recv()
    for z in range(chips):
        goal_sum[z] = (goal[away, z].astype(F32) + goal_in[z].astype(F32)).astype(BF16)
    for k in range(1, chips):
        remote(goal_sum.at[other(k)], goal_far.at[chip], far_send, far_recv, other(k) * 2 + away).start()
    remote(goal_sum.at[chip], goal_far.at[chip], far_send, far_recv, partner).start()

    def finish(a):
        remote(slots.at[a, core], slots.at[a, core], fw_send, fw_recv.at[a], partner).wait_recv()
        for z in range(chips):
            both = jnp.concatenate([slots[a, 0, z].astype(F32), slots[a, 1, z].astype(F32)], axis=0)
            hid_ref[2 * rows * z:2 * rows * (z + 1), a * span:(a + 1) * span] = both.astype(BF16)
        term = jnp.dot(
            hid_ref[:, a * span:(a + 1) * span], w_v[a * span:(a + 1) * span, :], preferred_element_type=F32
        )
        if a == 0:
            e_v[...] = term
        else:
            e_v[...] += term

    for a in range(pieces):
        there = slots.at[a, away, pl.ds(0, chips - 1)]
        remote(there, there, ag_send, ag_recv.at[a], partner).wait_recv()
        for k in range(1, chips):
            there = slots.at[a, away, other(k)]
            remote(there, there, fw_send, fw_recv.at[a], partner).start()
        if a > 0:
            finish(a - 1)
    finish(pieces - 1)

    logits = e_v[...]
    hits = lax.broadcasted_iota(jnp.int32, (tokens, width), 1).astype(F32) == aim_ref[:, 0:1]
    local_top = jnp.max(logits, axis=1, keepdims=True)
    expo = jnp.exp(logits - local_top)
    e_v[...] = expo
    g_ref[...] = jnp.where(hits, 0.0, expo).astype(BF16)
    local_total = jnp.sum(expo, axis=1, keepdims=True)
    local_picked = jnp.sum(jnp.where(hits, logits, 0.0), axis=1, keepdims=True)
    lane = lax.broadcasted_iota(jnp.int32, (tokens, 128), 1)
    packed = jnp.where(lane == 0, local_top, jnp.where(lane == 1, local_total, local_picked))
    near[0] = packed
    near_copy = remote(near.at[0], near.at[1], near_send, near_recv, partner)
    near_copy.start()
    stats[me] = jnp.transpose(packed)[0:8, :]
    for k in range(1, n):
        remote(stats.at[me], stats.at[me], st_send, st_recv, lax.rem(me + k, n)).start()

    def pair_copy(j):
        at = pl.ds(starts[j], widths[j])
        return remote(part.at[core, :, :, at], xbuf.at[:, :, at], x_send, x_recv.at[j], partner)

    def chip_sum(z, at):
        return part[away, z, :, at] * scale[0, away, z][:, 0:1] + xbuf[z, :, at] * scale[1, away, z][:, 0:1]

    def pass_on(j):
        at = slice(starts[j], starts[j] + widths[j])
        pair_copy(j).wait_recv()
        for z in range(chips):
            outb[z, :, at] = chip_sum(z, at).astype(BF16)
        at = pl.ds(starts[j], widths[j])
        for k in range(1, chips):
            remote(outb.at[other(k), :, at], rbuf.at[chip, :, at], rs_send, rs_recv, other(k) * 2 + away).start()
        remote(outb.at[chip, :, at], rbuf.at[chip, :, at], rs_send, rs_recv, partner).start()

    for j in range(len(widths)):
        if j == turn:
            near_copy.wait_recv()
            near_top = near[1][:, 0:1]
            chip_top = jnp.maximum(local_top, near_top)
            for i, own in enumerate((local_top, near_top)):
                spread = jnp.broadcast_to(jnp.exp(own - chip_top), (tokens, 128))
                for z in range(chips):
                    for half in range(2):
                        at = (2 * z + half) * rows
                        scale[i, half, z] = spread[at:at + rows, :]
        term = jnp.dot(g_ref[...], turned_v[:, starts[j]:starts[j] + widths[j]], preferred_element_type=F32)
        for z in range(chips):
            for half in range(2):
                at = (2 * z + half) * rows
                part[half, z, :, starts[j]:starts[j] + widths[j]] = term[at:at + rows, :]
        pair_copy(j).start()
        for i in after[j]:
            pass_on(i)

    remote(stats.at[pl.ds(0, n - 1)], stats.at[pl.ds(0, n - 1)], st_send, st_recv, partner).wait_recv()

    top = stats[0, 0:1, :]
    for k in range(1, n):
        top = jnp.maximum(top, stats[k, 0:1, :])
    total = jnp.zeros_like(top)
    picked = jnp.zeros_like(top)
    for k in range(n):
        total += stats[k, 1:2, :] * jnp.exp(stats[k, 0:1, :] - top)
        picked += stats[k, 2:3, :]
    loss_ref[...] = jnp.broadcast_to(jnp.sum(top + jnp.log(total) - picked, axis=1, keepdims=True) / tokens, loss_ref.shape)

    sub = lax.broadcasted_iota(jnp.int32, (128, tokens), 0)
    turned = jnp.where(sub == chips, jnp.exp(picked - top) / total - 1.0, jnp.where(sub == chips + 1, top, total))
    for z in range(chips):
        chip_top = jnp.maximum(stats[2 * z, 0:1, :], stats[2 * z + 1, 0:1, :])
        turned = jnp.where(sub == z, jnp.exp(chip_top - top) / total, turned)
    turned = jnp.transpose(turned)
    for k in range(n):
        mix[k] = turned[k * rows:(k + 1) * rows, :]
    factor = jnp.exp(local_top - turned[:, chips + 1:chips + 2]) / turned[:, chips + 2:chips + 3]
    hits = lax.broadcasted_iota(jnp.int32, (tokens, width), 1).astype(F32) == aim_ref[:, 0:1]
    g_ref[...] = (e_v[...] * factor - hits.astype(F32)).astype(BF16)

    for b in range(blocks):
        dw_ref[b * tall:(b + 1) * tall, :] = lax.dot_general(
            hid_ref[:, b * tall:(b + 1) * tall], g_ref[...], DOWN, preferred_element_type=F32
        ).astype(BF16)

    mine = mix[me]
    remote(goal_far, goal_far, far_send, far_recv, partner).wait_recv()
    remote(rbuf, rbuf, rs_send, rs_recv, partner).wait_recv()
    for b in range(blocks):
        at = slice(b * tall, (b + 1) * tall)
        goals = jnp.zeros((rows, tall), F32)
        summed = jnp.zeros((rows, tall), F32)
        for z in range(chips):
            summed += rbuf[z, :, at].astype(F32) * mine[:, z:z + 1]
            goals += goal_far[z, :, at].astype(F32)
        dh_ref[:, at] = (summed + goals * mine[:, chips:chips + 1]).astype(BF16)

    for ref, sem in (
        (slots.at[:, 0], ag_send), (slots.at[:, 0, pl.ds(0, chips - 1)], fw_send), (stats.at[pl.ds(0, n - 1)], st_send),
        (near.at[0], near_send), (xbuf, x_send), (rbuf, rs_send), (goal_in, goal_send), (goal_far, far_send),
    ):
        remote(ref, ref, sem, st_recv, partner).wait_send()


def store_kernel(dw_v, dh_v, loss_v, dw_hbm, dh_hbm, loss_hbm, one_v, sem):
    one_v[...] = loss_v[0:1, 0:1]
    copies = []
    count = sem.shape[0] - 2
    tall = dw_v.shape[0] // count
    for b in range(count):
        at = pl.ds(b * tall, tall)
        copies.append(pltpu.make_async_copy(dw_v.at[at, :], dw_hbm.at[at, :], sem.at[2 + b]))
    copies.append(pltpu.make_async_copy(dh_v, dh_hbm, sem.at[0]))
    copies.append(pltpu.make_async_copy(one_v, loss_hbm, sem.at[1]))
    for copy in copies:
        copy.start()
    for copy in copies:
        copy.wait()


def body(n, hidden, weight, targets):
    rows, depth = hidden.shape
    width = weight.shape[1]
    tokens = rows * n
    chips = n // 2
    pieces = split(depth, 3, 256)
    unit = depth // split(depth, 12, 128)
    widths, turn, after = plan(depth // unit)
    widths = [w * unit for w in widths]
    span = depth // pieces
    vmem = pl.BlockSpec(memory_space=pltpu.VMEM)
    dma = pltpu.SemaphoreType.DMA
    hbm = pl.BlockSpec(memory_space=pltpu.HBM)
    shared = (jax.ShapeDtypeStruct((depth, width), BF16), jax.ShapeDtypeStruct((rows, depth), BF16))
    tile = jax.ShapeDtypeStruct((8, 128), F32)
    held = pl.pallas_call(
        functools.partial(loss_kernel, n, widths, turn, after),
        out_shape=(*shared, tile),
        in_specs=[hbm, hbm, hbm],
        out_specs=(vmem, vmem, vmem),
        scratch_shapes=[
            pltpu.VMEM((1, tokens), jnp.int32),
            pltpu.VMEM((tokens, 128), F32),
            pltpu.VMEM((tokens, depth), BF16),
            pltpu.VMEM((tokens, width), BF16),
            pltpu.VMEM((depth, width), BF16),
            pltpu.VMEM((width, depth), BF16),
            pltpu.VMEM((pieces, 2, chips, rows, span), BF16),
            pltpu.VMEM((tokens, width), F32),
            pltpu.VMEM((n, 8, tokens), F32),
            pltpu.VMEM((2, tokens, 128), F32),
            pltpu.VMEM((2, 2, chips, rows, 128), F32),
            pltpu.VMEM((n, rows, 128), F32),
            pltpu.VMEM((2, chips, rows, depth), F32),
            pltpu.VMEM((chips, rows, depth), F32),
            pltpu.VMEM((chips, rows, depth), BF16),
            pltpu.VMEM((chips, rows, depth), BF16),
            pltpu.VMEM((2, chips, rows, depth), BF16),
            pltpu.VMEM((chips, rows, depth), BF16),
            pltpu.VMEM((chips, rows, depth), BF16),
            pltpu.VMEM((chips, rows, depth), BF16),
            dma((pieces + 1,)),
            dma((pieces,)),
            dma((8,)),
            dma((pieces,)),
            dma((pieces,)),
            dma((5,)),
            dma((len(widths),)),
        ],
        compiler_params=pltpu.CompilerParams(
            collective_id=0, has_side_effects=True, vmem_limit_bytes=45 * 1024 * 1024
        ),
    )(*[pltpu.with_memory_space_constraint(x, pltpu.HBM) for x in (hidden, weight, targets.reshape(1, tokens))])
    d_weight, d_hidden, loss = pl.pallas_call(
        store_kernel,
        out_shape=(*shared, jax.ShapeDtypeStruct((1, 1), F32)),
        in_specs=[vmem, vmem, vmem],
        out_specs=(hbm, hbm, hbm),
        scratch_shapes=[pltpu.VMEM((1, 1), F32), dma((2 + split(depth, 12, 16),))],
        compiler_params=pltpu.CompilerParams(vmem_limit_bytes=2 * 1024 * 1024),
    )(*held)
    return loss.reshape(1), d_hidden, d_weight


def solution(mesh):
    placed = (P(("dp", "vocab"), None), P(None, "vocab"), P("dp"))
    return jax.shard_map(
        functools.partial(body, mesh.shape["vocab"]),
        mesh=mesh,
        in_specs=placed,
        out_specs=(P("dp"), P(("dp", "vocab"), None), P("dp", "vocab")),
        check_vma=False,
    )
```

```python
import functools

import jax
import jax.numpy as jnp
from jax import lax
from jax.experimental import pallas as pl
from jax.experimental.pallas import tpu as pltpu
from jax.sharding import PartitionSpec as P

MESH = pl.DeviceIdType.MESH
F32 = jnp.float32
BF16 = jnp.bfloat16
DOWN = (((0,), (0,)), ((), ()))


def split(length, most, unit):
    for parts in range(most, 0, -1):
        if length % (parts * unit) == 0:
            return parts
    return 1


def plan(units):
    if units == 12:
        return [7, 5], 1, [[], [0, 1]]
    return [1] * units, 1, [[] if j == 0 else [j - 1] for j in range(units - 1)] + [[units - 2, units - 1] if units > 1 else [0]]


def remote(src, dst, send, recv, device):
    return pltpu.make_async_remote_copy(
        src_ref=src, dst_ref=dst, send_sem=send, recv_sem=recv, device_id={"vocab": device}, device_id_type=MESH
    )


def loss_kernel(
    n, spans, widths, turn, after, h_hbm, w_hbm, t_hbm, dw_ref, dh_ref, loss_ref,
    t_ref, aim_ref, hid_ref, g_ref, w_v, turned_v, slots, e_v, stats, near, scale, mix, part, xbuf, outb, rbuf,
    goal, goal_in, goal_sum, goal_far,
    in_sem, w_sem, send_sem, ag_recv, fw_recv, recv_sem, x_recv,
):
    me = lax.axis_index("vocab")
    chips = n // 2
    chip, core = me // 2, me % 2
    away = 1 - core
    partner = chip * 2 + away
    rows, pieces = slots.shape[2], len(spans)
    cuts = [sum(spans[:a]) for a in range(pieces)]
    tokens, width = e_v.shape
    depth = w_v.shape[0]
    blocks = split(depth, 6, 256)
    tall = depth // blocks
    starts = [sum(widths[:j]) for j in range(len(widths))]
    ag_send, fw_send, st_send, near_send, x_send, rs_send, goal_send, far_send = [send_sem.at[i] for i in range(8)]
    st_recv, near_recv, rs_recv, goal_recv, far_recv = [recv_sem.at[i] for i in range(5)]

    above = chips - 1 - chip

    def cols(a):
        return pl.ds(cuts[a], spans[a])

    def other(k):
        up = (above - k + chips) // chips
        return up * (chips - k) + (1 - up) * (k - 1 - above)

    takes = [
        pltpu.make_async_copy(h_hbm.at[:, cols(a)], slots.at[core, chip, :, cols(a)], in_sem.at[a])
        for a in range(pieces)
    ]
    takes.append(pltpu.make_async_copy(t_hbm, t_ref, in_sem.at[pieces]))
    for take in takes:
        take.start()
    loads = [
        pltpu.make_async_copy(w_hbm.at[cols(a), :], w_v.at[cols(a), :], w_sem.at[a])
        for a in range(pieces)
    ]

    barrier = pltpu.get_barrier_semaphore()
    for k in range(1, n):
        pl.semaphore_signal(barrier, inc=1, device_id={"vocab": lax.rem(me + k, n)}, device_id_type=MESH)
    for take in takes:
        take.wait()
    for load in loads:
        load.start()
    aim_ref[...] = jnp.transpose(jnp.broadcast_to((t_ref[...] - me * width).astype(F32), (128, tokens)))
    pl.semaphore_wait(barrier, n - 1)

    for a in range(pieces):
        own = slots.at[core, chip, :, cols(a)]
        for k in range(1, chips):
            remote(own, own, ag_send, ag_recv.at[a], other(k) * 2 + away).start()
        remote(own, own, ag_send, fw_recv.at[a], partner).start()

    hits = lax.broadcasted_iota(jnp.int32, (tokens, width), 1).astype(F32) == aim_ref[:, 0:1]
    g_ref[...] = hits.astype(F32).astype(BF16)
    for load in loads:
        load.wait()
    for b in range(blocks):
        turned_v[:, b * tall:(b + 1) * tall] = jnp.transpose(w_v[b * tall:(b + 1) * tall, :])
        term = jnp.dot(g_ref[...], turned_v[:, b * tall:(b + 1) * tall], preferred_element_type=F32)
        for z in range(chips):
            for half in range(2):
                at = (2 * z + half) * rows
                goal[half, z, :, b * tall:(b + 1) * tall] = term[at:at + rows, :].astype(BF16)
    goal_copy = remote(goal.at[core], goal_in, goal_send, goal_recv, partner)
    goal_copy.start()
    goal_copy.wait_recv()
    for z in range(chips):
        goal_sum[z] = (goal[away, z].astype(F32) + goal_in[z].astype(F32)).astype(BF16)
    for k in range(1, chips):
        remote(goal_sum.at[other(k)], goal_far.at[chip], far_send, far_recv, other(k) * 2 + away).start()
    remote(goal_sum.at[chip], goal_far.at[chip], far_send, far_recv, partner).start()

    def finish(a):
        at = slice(cuts[a], cuts[a] + spans[a])
        there = slots.at[core, :, :, cols(a)]
        remote(there, there, fw_send, fw_recv.at[a], partner).wait_recv()
        for z in range(chips):
            both = jnp.concatenate([slots[0, z, :, at].astype(F32), slots[1, z, :, at].astype(F32)], axis=0)
            hid_ref[2 * rows * z:2 * rows * (z + 1), at] = both.astype(BF16)
        term = jnp.dot(hid_ref[:, at], w_v[at, :], preferred_element_type=F32)
        if a == 0:
            e_v[...] = term
        else:
            e_v[...] += term

    for a in range(pieces):
        there = slots.at[away, pl.ds(0, chips - 1), :, cols(a)]
        remote(there, there, ag_send, ag_recv.at[a], partner).wait_recv()
        for k in range(1, chips):
            there = slots.at[away, other(k), :, cols(a)]
            remote(there, there, fw_send, fw_recv.at[a], partner).start()
        if a > 0:
            finish(a - 1)
    finish(pieces - 1)

    logits = e_v[...]
    hits = lax.broadcasted_iota(jnp.int32, (tokens, width), 1).astype(F32) == aim_ref[:, 0:1]
    local_top = jnp.max(logits, axis=1, keepdims=True)
    expo = jnp.exp(logits - local_top)
    e_v[...] = expo
    g_ref[...] = jnp.where(hits, 0.0, expo).astype(BF16)
    local_total = jnp.sum(expo, axis=1, keepdims=True)
    local_picked = jnp.sum(jnp.where(hits, logits, 0.0), axis=1, keepdims=True)
    lane = lax.broadcasted_iota(jnp.int32, (tokens, 128), 1)
    packed = jnp.where(lane == 0, local_top, jnp.where(lane == 1, local_total, local_picked))
    near[0] = packed
    near_copy = remote(near.at[0], near.at[1], near_send, near_recv, partner)
    near_copy.start()
    stats[me] = jnp.transpose(packed)[0:8, :]
    for k in range(1, n):
        remote(stats.at[me], stats.at[me], st_send, st_recv, lax.rem(me + k, n)).start()

    def pair_copy(j):
        at = pl.ds(starts[j], widths[j])
        return remote(part.at[core, :, :, at], xbuf.at[:, :, at], x_send, x_recv.at[j], partner)

    def chip_sum(z, at):
        return part[away, z, :, at] * scale[0, away, z][:, 0:1] + xbuf[z, :, at] * scale[1, away, z][:, 0:1]

    def pass_on(j):
        at = slice(starts[j], starts[j] + widths[j])
        pair_copy(j).wait_recv()
        for z in range(chips):
            outb[z, :, at] = chip_sum(z, at).astype(BF16)
        at = pl.ds(starts[j], widths[j])
        for k in range(1, chips):
            remote(outb.at[other(k), :, at], rbuf.at[chip, :, at], rs_send, rs_recv, other(k) * 2 + away).start()
        remote(outb.at[chip, :, at], rbuf.at[chip, :, at], rs_send, rs_recv, partner).start()

    for j in range(len(widths)):
        if j == turn:
            near_copy.wait_recv()
            near_top = near[1][:, 0:1]
            chip_top = jnp.maximum(local_top, near_top)
            for i, own in enumerate((local_top, near_top)):
                spread = jnp.broadcast_to(jnp.exp(own - chip_top), (tokens, 128))
                for z in range(chips):
                    for half in range(2):
                        at = (2 * z + half) * rows
                        scale[i, half, z] = spread[at:at + rows, :]
        term = jnp.dot(g_ref[...], turned_v[:, starts[j]:starts[j] + widths[j]], preferred_element_type=F32)
        for z in range(chips):
            for half in range(2):
                at = (2 * z + half) * rows
                part[half, z, :, starts[j]:starts[j] + widths[j]] = term[at:at + rows, :]
        pair_copy(j).start()
        for i in after[j]:
            pass_on(i)

    remote(stats.at[pl.ds(0, n - 1)], stats.at[pl.ds(0, n - 1)], st_send, st_recv, partner).wait_recv()

    top = stats[0, 0:1, :]
    for k in range(1, n):
        top = jnp.maximum(top, stats[k, 0:1, :])
    total = jnp.zeros_like(top)
    picked = jnp.zeros_like(top)
    for k in range(n):
        total += stats[k, 1:2, :] * jnp.exp(stats[k, 0:1, :] - top)
        picked += stats[k, 2:3, :]
    loss_ref[...] = jnp.broadcast_to(jnp.sum(top + jnp.log(total) - picked, axis=1, keepdims=True) / tokens, loss_ref.shape)

    sub = lax.broadcasted_iota(jnp.int32, (128, tokens), 0)
    turned = jnp.where(sub == chips, jnp.exp(picked - top) / total - 1.0, jnp.where(sub == chips + 1, top, total))
    for z in range(chips):
        chip_top = jnp.maximum(stats[2 * z, 0:1, :], stats[2 * z + 1, 0:1, :])
        turned = jnp.where(sub == z, jnp.exp(chip_top - top) / total, turned)
    turned = jnp.transpose(turned)
    for k in range(n):
        mix[k] = turned[k * rows:(k + 1) * rows, :]
    factor = jnp.exp(local_top - turned[:, chips + 1:chips + 2]) / turned[:, chips + 2:chips + 3]
    hits = lax.broadcasted_iota(jnp.int32, (tokens, width), 1).astype(F32) == aim_ref[:, 0:1]
    g_ref[...] = (e_v[...] * factor - hits.astype(F32)).astype(BF16)

    for b in range(blocks):
        dw_ref[b * tall:(b + 1) * tall, :] = lax.dot_general(
            hid_ref[:, b * tall:(b + 1) * tall], g_ref[...], DOWN, preferred_element_type=F32
        ).astype(BF16)

    mine = mix[me]
    remote(goal_far, goal_far, far_send, far_recv, partner).wait_recv()
    remote(rbuf, rbuf, rs_send, rs_recv, partner).wait_recv()
    for b in range(blocks):
        at = slice(b * tall, (b + 1) * tall)
        goals = jnp.zeros((rows, tall), F32)
        summed = jnp.zeros((rows, tall), F32)
        for z in range(chips):
            summed += rbuf[z, :, at].astype(F32) * mine[:, z:z + 1]
            goals += goal_far[z, :, at].astype(F32)
        dh_ref[:, at] = (summed + goals * mine[:, chips:chips + 1]).astype(BF16)

    for ref, sem in (
        (slots.at[0], ag_send), (slots.at[0, pl.ds(0, chips - 1)], fw_send), (stats.at[pl.ds(0, n - 1)], st_send),
        (near.at[0], near_send), (xbuf, x_send), (rbuf, rs_send), (goal_in, goal_send), (goal_far, far_send),
    ):
        remote(ref, ref, sem, st_recv, partner).wait_send()


def store_kernel(dw_v, dh_v, loss_v, dw_hbm, dh_hbm, loss_hbm, one_v, sem):
    one_v[...] = loss_v[0:1, 0:1]
    copies = []
    count = sem.shape[0] - 2
    tall = dw_v.shape[0] // count
    for b in range(count):
        at = pl.ds(b * tall, tall)
        copies.append(pltpu.make_async_copy(dw_v.at[at, :], dw_hbm.at[at, :], sem.at[2 + b]))
    copies.append(pltpu.make_async_copy(dh_v, dh_hbm, sem.at[0]))
    copies.append(pltpu.make_async_copy(one_v, loss_hbm, sem.at[1]))
    for copy in copies:
        copy.start()
    for copy in copies:
        copy.wait()


def body(n, hidden, weight, targets):
    rows, depth = hidden.shape
    width = weight.shape[1]
    tokens = rows * n
    chips = n // 2
    unit = depth // split(depth, 12, 128)
    widths, turn, after = plan(depth // unit)
    widths = [w * unit for w in widths]
    spans = [5 * unit, 5 * unit, 2 * unit] if depth == 12 * unit else [depth]
    pieces = len(spans)
    vmem = pl.BlockSpec(memory_space=pltpu.VMEM)
    dma = pltpu.SemaphoreType.DMA
    hbm = pl.BlockSpec(memory_space=pltpu.HBM)
    shared = (jax.ShapeDtypeStruct((depth, width), BF16), jax.ShapeDtypeStruct((rows, depth), BF16))
    tile = jax.ShapeDtypeStruct((8, 128), F32)
    held = pl.pallas_call(
        functools.partial(loss_kernel, n, spans, widths, turn, after),
        out_shape=(*shared, tile),
        in_specs=[hbm, hbm, hbm],
        out_specs=(vmem, vmem, vmem),
        scratch_shapes=[
            pltpu.VMEM((1, tokens), jnp.int32),
            pltpu.VMEM((tokens, 128), F32),
            pltpu.VMEM((tokens, depth), BF16),
            pltpu.VMEM((tokens, width), BF16),
            pltpu.VMEM((depth, width), BF16),
            pltpu.VMEM((width, depth), BF16),
            pltpu.VMEM((2, chips, rows, depth), BF16),
            pltpu.VMEM((tokens, width), F32),
            pltpu.VMEM((n, 8, tokens), F32),
            pltpu.VMEM((2, tokens, 128), F32),
            pltpu.VMEM((2, 2, chips, rows, 128), F32),
            pltpu.VMEM((n, rows, 128), F32),
            pltpu.VMEM((2, chips, rows, depth), F32),
            pltpu.VMEM((chips, rows, depth), F32),
            pltpu.VMEM((chips, rows, depth), BF16),
            pltpu.VMEM((chips, rows, depth), BF16),
            pltpu.VMEM((2, chips, rows, depth), BF16),
            pltpu.VMEM((chips, rows, depth), BF16),
            pltpu.VMEM((chips, rows, depth), BF16),
            pltpu.VMEM((chips, rows, depth), BF16),
            dma((pieces + 1,)),
            dma((pieces,)),
            dma((8,)),
            dma((pieces,)),
            dma((pieces,)),
            dma((5,)),
            dma((len(widths),)),
        ],
        compiler_params=pltpu.CompilerParams(
            collective_id=0, has_side_effects=True, vmem_limit_bytes=45 * 1024 * 1024
        ),
    )(*[pltpu.with_memory_space_constraint(x, pltpu.HBM) for x in (hidden, weight, targets.reshape(1, tokens))])
    d_weight, d_hidden, loss = pl.pallas_call(
        store_kernel,
        out_shape=(*shared, jax.ShapeDtypeStruct((1, 1), F32)),
        in_specs=[vmem, vmem, vmem],
        out_specs=(hbm, hbm, hbm),
        scratch_shapes=[pltpu.VMEM((1, 1), F32), dma((2 + split(depth, 12, 16),))],
        compiler_params=pltpu.CompilerParams(vmem_limit_bytes=2 * 1024 * 1024),
    )(*held)
    return loss.reshape(1), d_hidden, d_weight


def solution(mesh):
    placed = (P(("dp", "vocab"), None), P(None, "vocab"), P("dp"))
    return jax.shard_map(
        functools.partial(body, mesh.shape["vocab"]),
        mesh=mesh,
        in_specs=placed,
        out_specs=(P("dp"), P(("dp", "vocab"), None), P("dp", "vocab")),
        check_vma=False,
    )
```
